32 devices in a mesh: rows: 8 (over z, y), tp: 4 (over x, core).
Axes of the slice: x: 2, y: 2, z: 4, core: 2. Of those that a mesh axis runs over, the one named last changes fastest.
Arguments:
- train_gate: bfloat16 [2560, 9728], P('rows', 'tp'), may hold values from -0.125 to 0.125
- low_gate: bfloat16 [2560, 16], P('rows'), may hold values from -0.125 to 0.125
- high_gate: bfloat16 [16, 9728], P(None, 'tp'), may hold values from -1.5 to 1.5
- train_up: bfloat16 [2560, 9728], P('rows', 'tp'), may hold values from -0.125 to 0.125
- low_up: bfloat16 [2560, 16], P('rows'), may hold values from -0.125 to 0.125
- high_up: bfloat16 [16, 9728], P(None, 'tp'), may hold values from -1.5 to 1.5
- train_down: bfloat16 [9728, 2560], P('tp', 'rows'), may hold values from -0.0625 to 0.0625
- low_down: bfloat16 [9728, 16], P('tp'), may hold values from -0.0625 to 0.0625
- high_down: bfloat16 [16, 2560], P(None, 'rows'), may hold values from -1.5 to 1.5
- norm_train: float32 [2560], P(('rows', 'tp')), may hold values from 0.25 to 1.75
- norm_step: float32 [2560], P(('rows', 'tp')), may hold values from -0.3 to 0.3
Outputs:
- serve_gate: bfloat16 [9728, 2560], P('tp')
- serve_up: bfloat16 [9728, 2560], P('tp')
- serve_down: bfloat16 [2560, 9728], P(None, 'tp')
- serve_norm: bfloat16 [2560], replicated
The draws below stay inside these ranges and needn't reach their ends.
All inputs are finite; a program needn't handle non-finite values.
Results may differ from the reference program's by a relative error of at most 0.001.
Values may be sent and summed in bfloat16 or wider, within the bound.
A program may use at most 128 MiB of HBM per device.

```python
import jax
import jax.numpy as jnp

D_MODEL = 2560
D_INNER = 9728
RANK = 16


def block_scale(own_key, dims, pieces, low, largest):
    level, own = 1.0, jax.random.fold_in(own_key, 6)
    for axis_at, shards_of in pieces:
        heights = jnp.exp(jax.random.uniform(jax.random.fold_in(own, axis_at), (shards_of,), jnp.float32, low / len(pieces), largest / len(pieces)))
        level = level * jnp.repeat(heights, dims[axis_at] // shards_of).reshape([-1 if axis == axis_at else 1 for axis in range(len(dims))])
    return level


def normal_values(own_key, extent, scale, bound, shards=(), kind=jnp.bfloat16):
    entries = scale * jax.random.normal(own_key, extent, jnp.float32)
    if shards:
        entries = entries * block_scale(own_key, extent, shards, -0.22, 0.18)
    return jnp.clip(entries, -bound, bound).astype(kind)


def setup_inputs(seed: int = 0) -> dict:
    splits = jax.random.split(jax.random.key(seed), 12)
    train_gate = normal_values(splits[0], (D_MODEL, D_INNER), D_MODEL ** -0.5, 0.125, ((0, 8), (1, 4)))
    low_gate = normal_values(splits[1], (D_MODEL, RANK), D_MODEL ** -0.5, 0.125, ((0, 8),))
    high_gate = normal_values(splits[2], (RANK, D_INNER), RANK ** -0.5, 1.5, ((1, 4),))
    train_up = normal_values(splits[3], (D_MODEL, D_INNER), D_MODEL ** -0.5, 0.125, ((0, 8), (1, 4)))
    low_up = normal_values(splits[4], (D_MODEL, RANK), D_MODEL ** -0.5, 0.125, ((0, 8),))
    high_up = normal_values(splits[5], (RANK, D_INNER), RANK ** -0.5, 1.5, ((1, 4),))
    train_down = normal_values(splits[6], (D_INNER, D_MODEL), D_INNER ** -0.5, 0.0625, ((0, 4), (1, 8)))
    low_down = normal_values(splits[7], (D_INNER, RANK), D_INNER ** -0.5, 0.0625, ((0, 4),))
    high_down = normal_values(splits[8], (RANK, D_MODEL), RANK ** -0.5, 1.5, ((1, 8),))
    norm_train = jnp.clip(1.0 + 0.15 * jax.random.normal(splits[9], (D_MODEL,), jnp.float32), 0.25, 1.75)
    norm_step = jnp.clip(jax.random.uniform(splits[10], (D_MODEL,), jnp.float32, -0.3, 0.3) * block_scale(splits[10], (D_MODEL,), ((0, 32),), -0.4, 0.0), -0.3, 0.3)
    return {"train_gate": train_gate, "low_gate": low_gate, "high_gate": high_gate, "train_up": train_up, "low_up": low_up, "high_up": high_up, "train_down": train_down, "low_down": low_down, "high_down": high_down, "norm_train": norm_train, "norm_step": norm_step}


mix_rate = 1.0


def reference(train_gate, low_gate, high_gate, train_up, low_up, high_up, train_down, low_down, high_down, norm_train, norm_step):
    fresh_gate = train_gate.astype(jnp.float32) + mix_rate * jnp.dot(low_gate, high_gate, preferred_element_type=jnp.float32)
    fresh_up = train_up.astype(jnp.float32) + mix_rate * jnp.dot(low_up, high_up, preferred_element_type=jnp.float32)
    fresh_down = train_down.astype(jnp.float32) + mix_rate * jnp.dot(low_down, high_down, preferred_element_type=jnp.float32)
    serve_gate = fresh_gate.T.astype(jnp.bfloat16)
    serve_up = fresh_up.T.astype(jnp.bfloat16)
    serve_down = fresh_down.T.astype(jnp.bfloat16)
    serve_norm = (norm_train + norm_step).astype(jnp.bfloat16)
    return serve_gate, serve_up, serve_down, serve_norm
```

```python
import functools

import jax
import jax.numpy as jnp
from jax import lax
from jax.experimental import pallas as pl
from jax.experimental.pallas import tpu as pltpu
from jax.sharding import PartitionSpec as P

mix_rate = 1.0
PARTS = 2


def torus_of(rows):
    y = 1
    while y * y * 4 <= rows and rows % (y * 2) == 0:
        y *= 2
    return rows // y, y


def make_plan(depth, width, halved, parts):
    plan = []
    for dz in sorted(range(1 - depth, depth), key=abs):
        toward = (dz > 0) - (dz < 0)
        for dy in range(width):
            for part in range(parts) if (dz, dy) != (0, 0) else ():
                by_y = dy > 0 and (abs(dz) != 1 or part in halved)
                plan.append((dz, dy, part, (0, 1) if by_y else (toward, 0)))
    return plan


def gather_kernel(depth, width, tp, *refs):
    owns, norm_ref, outs, norm_out = refs[:3], refs[3], refs[4:7], refs[7]
    send, recv, tp_send, tp_recv, own_sem, kept, in_sem, out_sem = refs[8:]
    me, me_tp = lax.axis_index("rows"), lax.axis_index("tp")
    z, y = me // width, lax.rem(me, width)
    block = owns[0].shape[0]
    share = block // PARTS

    entries = []
    for array in range(4):
        parts, halved = (PARTS, (array % PARTS,)) if array < 3 else (1, (0,))
        for entry in make_plan(depth, width, halved, parts):
            entries.append((array, *entry))
    index = {e[:4]: n for n, e in enumerate(entries)}
    slot = 3 * PARTS

    def piece(array, dz, dy, part):
        row = (z + dz) * width + lax.rem(y + dy, width)
        if array == 3:
            return norm_out.at[row], norm_out.at[row]
        start = pl.multiple_of(row * block + part * share, 8)
        place = outs[array].at[pl.ds(start, share), :]
        if (dz, dy) == (0, 0):
            return owns[array].at[pl.ds(part * share, share), :], place
        return place, place

    def sending(entry):
        array, dz, dy, part, (sz, sy) = entry
        source, place = piece(array, dz - sz, dy - sy, part)
        exists = jnp.logical_and(z - sz >= 0, z - sz < depth)
        exists = jnp.logical_and(
            exists, jnp.logical_and(z - sz + dz >= 0, z - sz + dz < depth)
        )
        to = lax.rem(z - sz + depth, depth) * width + lax.rem(y - sy + width, width)
        n = index[array, dz, dy, part]
        copy = pltpu.make_async_remote_copy(
            src_ref=source,
            dst_ref=place,
            send_sem=send.at[n],
            recv_sem=recv.at[n],
            device_id=(to, me_tp),
            device_id_type=pl.DeviceIdType.MESH,
        )
        return copy, exists

    def start(entry):
        copy, exists = sending(entry)

        @pl.when(exists)
        def _():
            copy.start()

    def arrived(entry):
        array, dz, dy, part, _ = entry
        _, place = piece(array, dz, dy, part)
        n = index[array, dz, dy, part]

        @pl.when(jnp.logical_and(z + dz >= 0, z + dz < depth))
        def _():
            pltpu.make_async_remote_copy(
                src_ref=place,
                dst_ref=place,
                send_sem=send.at[n],
                recv_sem=recv.at[n],
                device_id=(me, me_tp),
                device_id_type=pl.DeviceIdType.MESH,
            ).wait_recv()

    barrier = pltpu.get_barrier_semaphore()
    up, down = z + 1 < depth, z > 0
    for there, exists in ((me + width, up), (me - width, down)):

        @pl.when(exists)
        def _():
            pl.semaphore_signal(
                barrier, inc=1, device_id=(there, me_tp), device_id_type=pl.DeviceIdType.MESH
            )

    sides = {1 % width, (width - 1) % width} - {0}
    for side in sorted(sides):
        there = z * width + lax.rem(y + side, width)
        pl.semaphore_signal(
            barrier, inc=1, device_id=(there, me_tp), device_id_type=pl.DeviceIdType.MESH
        )
    for k in range(1, tp):
        there = lax.rem(me_tp + k, tp)
        pl.semaphore_signal(
            barrier, inc=1, device_id=(me, there), device_id_type=pl.DeviceIdType.MESH
        )
    pl.semaphore_wait(
        barrier, up.astype(jnp.int32) + down.astype(jnp.int32) + len(sides) + tp - 1
    )

    own_copy = pltpu.make_async_copy(norm_ref, norm_out.at[me, me_tp], own_sem)
    own_copy.start()

    def across(k, here):
        return pltpu.make_async_remote_copy(
            src_ref=norm_ref,
            dst_ref=norm_out.at[me, here],
            send_sem=tp_send.at[k - 1],
            recv_sem=tp_recv.at[k - 1],
            device_id=(me, lax.rem(me_tp + k, tp)),
            device_id_type=pl.DeviceIdType.MESH,
        )

    for k in range(1, tp):
        across(k, me_tp).start()

    events = []
    for n, entry in enumerate(entries):
        array, dz, dy, part, (sz, sy) = entry
        turn = array * PARTS + part
        late = sz != 0 and dy != 0
        parent = (array, dz - sz, dy - sy, part)
        if parent[1:3] == (0, 0):
            events.append((-1, turn, n, start, entry))
        elif late:
            events.append((slot * (depth - 2 + (dy - 1) * depth) + slot, 0, n, start, entry))
        if late:
            key = slot * (depth * dy)
        elif sy:
            key = slot * (abs(dz) + (dy - 1) * depth)
        else:
            key = slot * (abs(dz) - 1)
        events.append((key + turn, 1, n, arrived, entry))
        for child in entries:
            if (
                child[0] == array
                and child[3] == part
                and (child[1] - child[4][0], child[2] - child[4][1]) == (dz, dy)
                and not (child[4][0] and child[2])
            ):
                events.append((key + turn, 2, n, start, child))

    ins = [
        pltpu.make_async_copy(own, kept.at[n], in_sem.at[n]) for n, own in enumerate(owns)
    ]
    mine = pl.ds(pl.multiple_of(me * block, 8), block)
    keeps = [
        pltpu.make_async_copy(kept.at[n], out.at[mine, :], out_sem.at[n])
        for n, out in enumerate(outs)
    ]
    own_done = False
    for event in sorted(events, key=lambda e: e[:3]):
        if not own_done and event[4][0] == 3:
            own_copy.wait()
            for copy in ins:
                copy.start()
            for into, copy in zip(ins, keeps):
                into.wait()
                copy.start()
            for k in range(1, tp):
                across(k, lax.rem(me_tp - k + tp, tp)).wait_recv()
            own_done = True
        event[3](event[4])

    for copy in keeps:
        copy.wait()
    for k in range(1, tp):
        across(k, me_tp).wait_send()
    for entry in entries:
        copy, exists = sending(entry)

        @pl.when(exists)
        def _():
            copy.wait_send()


def gather(owns, norm, rows, tp):
    depth, width = torus_of(rows)
    block, columns = owns[0].shape
    count = sum(len(make_plan(depth, width, (0,), p)) for p in (PARTS,) * 3 + (1,))
    any_spec = pl.BlockSpec(memory_space=pl.ANY)
    whole = jax.ShapeDtypeStruct((block * rows, columns), jnp.bfloat16)
    norms = jax.ShapeDtypeStruct((rows, tp) + norm.shape, jnp.bfloat16)
    return pl.pallas_call(
        functools.partial(gather_kernel, depth, width, tp),
        out_shape=(whole, whole, whole, norms),
        in_specs=[any_spec] * 4,
        out_specs=(any_spec,) * 4,
        scratch_shapes=[
            pltpu.SemaphoreType.DMA((count,)),
            pltpu.SemaphoreType.DMA((count,)),
            pltpu.SemaphoreType.DMA((tp - 1,)),
            pltpu.SemaphoreType.DMA((tp - 1,)),
            pltpu.SemaphoreType.DMA,
            pltpu.VMEM((3, block, columns), jnp.bfloat16),
            pltpu.SemaphoreType.DMA((3,)),
            pltpu.SemaphoreType.DMA((3,)),
        ],
        compiler_params=pltpu.CompilerParams(collective_id=0, has_side_effects=True),
    )(*owns, norm)


def body(
    rows,
    tp,
    train_gate,
    low_gate,
    high_gate,
    train_up,
    low_up,
    high_up,
    train_down,
    low_down,
    high_down,
    norm_train,
    norm_step,
):
    own_gate = (
        train_gate.astype(jnp.float32)
        + mix_rate * jnp.dot(low_gate, high_gate, preferred_element_type=jnp.float32)
    ).astype(jnp.bfloat16)
    own_up = (
        train_up.astype(jnp.float32)
        + mix_rate * jnp.dot(low_up, high_up, preferred_element_type=jnp.float32)
    ).astype(jnp.bfloat16)
    own_down = (
        train_down.astype(jnp.float32)
        + mix_rate * jnp.dot(low_down, high_down, preferred_element_type=jnp.float32)
    ).astype(jnp.bfloat16)
    owns = (own_gate, own_up, own_down.T)
    norm = (norm_train + norm_step).astype(jnp.bfloat16)[None]
    gate, up, down, norms = gather(owns, norm, rows, tp)
    return (gate.T, up.T, down, norms.reshape(-1))


def solution(mesh):
    in_specs = (
        P("rows", "tp"),
        P("rows", None),
        P(None, "tp"),
        P("rows", "tp"),
        P("rows", None),
        P(None, "tp"),
        P("tp", "rows"),
        P("tp", None),
        P(None, "rows"),
        P(("rows", "tp")),
        P(("rows", "tp")),
    )
    out_specs = (P("tp", None), P("tp", None), P(None, "tp"), P())
    return jax.shard_map(
        functools.partial(body, mesh.shape["rows"], mesh.shape["tp"]),
        mesh=mesh,
        in_specs=in_specs,
        out_specs=out_specs,
        check_vma=False,
    )
```

```python
import functools

import jax
import jax.numpy as jnp
from jax import lax
from jax.experimental import pallas as pl
from jax.experimental.pallas import tpu as pltpu
from jax.sharding import PartitionSpec as P

mix_rate = 1.0
PARTS = 2


def torus_of(rows):
    y = 1
    while y * y * 4 <= rows and rows % (y * 2) == 0:
        y *= 2
    return rows // y, y


def make_plan(depth, width, halved, parts):
    plan = []
    for dz in sorted(range(1 - depth, depth), key=abs):
        toward = (dz > 0) - (dz < 0)
        for dy in range(width):
            for part in range(parts) if (dz, dy) != (0, 0) else ():
                by_y = dy > 0 and (abs(dz) != 1 or part in halved)
                plan.append((dz, dy, part, (0, 1) if by_y else (toward, 0)))
    return plan


def gather_kernel(depth, width, tp, *refs):
    owns, norm_ref, outs, norm_out = refs[:3], refs[3], refs[4:7], refs[7]
    turned = refs[8:10]
    send, recv, tp_send, tp_recv, own_sem, kept, in_sem, out_sem, strip, strip_sem, over, over_sem = refs[10:]
    me, me_tp = lax.axis_index("rows"), lax.axis_index("tp")
    z, y = me // width, lax.rem(me, width)
    block = owns[0].shape[0]
    share = block // PARTS

    entries = []
    for array in range(4):
        parts, halved = (PARTS, (array % PARTS,)) if array < 3 else (1, (0,))
        for entry in make_plan(depth, width, halved, parts):
            entries.append((array, *entry))
    index = {e[:4]: n for n, e in enumerate(entries)}
    slot = 3 * PARTS

    def piece(array, dz, dy, part):
        row = (z + dz) * width + lax.rem(y + dy, width)
        if array == 3:
            return norm_out.at[row], norm_out.at[row]
        start = pl.multiple_of(row * block + part * share, 8)
        place = outs[array].at[pl.ds(start, share), :]
        if (dz, dy) == (0, 0):
            return owns[array].at[pl.ds(part * share, share), :], place
        return place, place

    def sending(entry):
        array, dz, dy, part, (sz, sy) = entry
        source, place = piece(array, dz - sz, dy - sy, part)
        exists = jnp.logical_and(z - sz >= 0, z - sz < depth)
        exists = jnp.logical_and(
            exists, jnp.logical_and(z - sz + dz >= 0, z - sz + dz < depth)
        )
        to = lax.rem(z - sz + depth, depth) * width + lax.rem(y - sy + width, width)
        n = index[array, dz, dy, part]
        copy = pltpu.make_async_remote_copy(
            src_ref=source,
            dst_ref=place,
            send_sem=send.at[n],
            recv_sem=recv.at[n],
            device_id=(to, me_tp),
            device_id_type=pl.DeviceIdType.MESH,
        )
        return copy, exists

    def start(entry):
        copy, exists = sending(entry)

        @pl.when(exists)
        def _():
            copy.start()

    def arrived(entry):
        array, dz, dy, part, _ = entry
        _, place = piece(array, dz, dy, part)
        n = index[array, dz, dy, part]

        @pl.when(jnp.logical_and(z + dz >= 0, z + dz < depth))
        def _():
            pltpu.make_async_remote_copy(
                src_ref=place,
                dst_ref=place,
                send_sem=send.at[n],
                recv_sem=recv.at[n],
                device_id=(me, me_tp),
                device_id_type=pl.DeviceIdType.MESH,
            ).wait_recv()

    barrier = pltpu.get_barrier_semaphore()
    up, down = z + 1 < depth, z > 0
    for there, exists in ((me + width, up), (me - width, down)):

        @pl.when(exists)
        def _():
            pl.semaphore_signal(
                barrier, inc=1, device_id=(there, me_tp), device_id_type=pl.DeviceIdType.MESH
            )

    sides = {1 % width, (width - 1) % width} - {0}
    for side in sorted(sides):
        there = z * width + lax.rem(y + side, width)
        pl.semaphore_signal(
            barrier, inc=1, device_id=(there, me_tp), device_id_type=pl.DeviceIdType.MESH
        )
    for k in range(1, tp):
        there = lax.rem(me_tp + k, tp)
        pl.semaphore_signal(
            barrier, inc=1, device_id=(me, there), device_id_type=pl.DeviceIdType.MESH
        )
    pl.semaphore_wait(
        barrier, up.astype(jnp.int32) + down.astype(jnp.int32) + len(sides) + tp - 1
    )

    own_copy = pltpu.make_async_copy(norm_ref, norm_out.at[me, me_tp], own_sem)
    own_copy.start()

    def across(k, here):
        return pltpu.make_async_remote_copy(
            src_ref=norm_ref,
            dst_ref=norm_out.at[me, here],
            send_sem=tp_send.at[k - 1],
            recv_sem=tp_recv.at[k - 1],
            device_id=(me, lax.rem(me_tp + k, tp)),
            device_id_type=pl.DeviceIdType.MESH,
        )

    for k in range(1, tp):
        across(k, me_tp).start()

    events, leaves = [], ([], [], [], [])
    for n, entry in enumerate(entries):
        array, dz, dy, part, (sz, sy) = entry
        turn = array * PARTS + part
        late = sz != 0 and dy != 0
        parent = (array, dz - sz, dy - sy, part)
        if parent[1:3] == (0, 0):
            events.append((-1, turn, n, start, entry))
        elif late:
            events.append((slot * (depth - 2 + (dy - 1) * depth) + slot, 0, n, start, entry))
        if late:
            key = slot * (depth * dy)
        elif sy:
            key = slot * (abs(dz) + (dy - 1) * depth)
        else:
            key = slot * (abs(dz) - 1)
        children = []
        for child in entries:
            if (
                child[0] == array
                and child[3] == part
                and (child[1] - child[4][0], child[2] - child[4][1]) == (dz, dy)
            ):
                children.append(child)
        if not children:
            leaves[array].append((key + turn, n, entry))
            continue
        events.append((key + turn, 1, n, arrived, entry))
        for child in children:
            if not (child[4][0] and child[2]):
                events.append((key + turn, 2, n, start, child))

    ins = [
        pltpu.make_async_copy(own, kept.at[n], in_sem.at[n]) for n, own in enumerate(owns)
    ]
    mine = pl.ds(pl.multiple_of(me * block, 8), block)
    keeps = [
        pltpu.make_async_copy(kept.at[n], out.at[mine, :], out_sem.at[n])
        for n, out in enumerate(outs)
    ]
    own_done = False
    for event in sorted(events, key=lambda e: e[:3]):
        if not own_done and event[4][0] == 3:
            own_copy.wait()
            for copy in ins:
                copy.start()
            for into, copy in zip(ins, keeps):
                into.wait()
                copy.start()
            for k in range(1, tp):
                across(k, lax.rem(me_tp - k + tp, tp)).wait_recv()
            own_done = True
        event[3](event[4])

    for copy in keeps:
        copy.wait()
    chunk = strip.shape[1]

    def turn_over(array):
        def fetch(i, at):
            return pltpu.make_async_copy(
                outs[array].at[pl.ds(pl.multiple_of(i * chunk, chunk), chunk), :],
                strip.at[at],
                strip_sem.at[at],
            )

        def store(i, at):
            return pltpu.make_async_copy(
                over.at[at],
                turned[array].at[:, pl.ds(pl.multiple_of(i * chunk, chunk), chunk)],
                over_sem.at[at],
            )

        steps = outs[array].shape[0] // chunk
        fetch(0, 0).start()

        def one(i, carry):
            at = lax.rem(i, 2)

            @pl.when(i + 1 < steps)
            def _():
                fetch(i + 1, 1 - at).start()

            fetch(i, at).wait()

            @pl.when(i >= 2)
            def _():
                store(i - 2, at).wait()

            over[at] = strip[at].T
            store(i, at).start()
            return carry

        lax.fori_loop(0, steps, one, 0)
        for i in range(max(steps - 2, 0), steps):
            store(i, i % 2).wait()

    for array in range(4):
        for _, _, entry in sorted(leaves[array]):
            arrived(entry)
        if array < 2:
            turn_over(array)
    for k in range(1, tp):
        across(k, me_tp).wait_send()
    for entry in entries:
        copy, exists = sending(entry)

        @pl.when(exists)
        def _():
            copy.wait_send()


def gather(owns, norm, rows, tp):
    depth, width = torus_of(rows)
    block, columns = owns[0].shape
    count = sum(len(make_plan(depth, width, (0,), p)) for p in (PARTS,) * 3 + (1,))
    any_spec = pl.BlockSpec(memory_space=pl.ANY)
    whole = jax.ShapeDtypeStruct((block * rows, columns), jnp.bfloat16)
    norms = jax.ShapeDtypeStruct((rows, tp) + norm.shape, jnp.bfloat16)
    high = block * rows
    chunk = 256 if high % 256 == 0 else 128
    turned = jax.ShapeDtypeStruct((columns, high), jnp.bfloat16)
    return pl.pallas_call(
        functools.partial(gather_kernel, depth, width, tp),
        out_shape=(whole, whole, whole, norms, turned, turned),
        in_specs=[any_spec] * 4,
        out_specs=(any_spec,) * 6,
        scratch_shapes=[
            pltpu.SemaphoreType.DMA((count,)),
            pltpu.SemaphoreType.DMA((count,)),
            pltpu.SemaphoreType.DMA((tp - 1,)),
            pltpu.SemaphoreType.DMA((tp - 1,)),
            pltpu.SemaphoreType.DMA,
            pltpu.VMEM((3, block, columns), jnp.bfloat16),
            pltpu.SemaphoreType.DMA((3,)),
            pltpu.SemaphoreType.DMA((3,)),
            pltpu.VMEM((2, chunk, columns), jnp.bfloat16),
            pltpu.SemaphoreType.DMA((2,)),
            pltpu.VMEM((2, columns, chunk), jnp.bfloat16),
            pltpu.SemaphoreType.DMA((2,)),
        ],
        compiler_params=pltpu.CompilerParams(
            collective_id=0, has_side_effects=True
        ),
    )(*owns, norm)


def body(
    rows,
    tp,
    train_gate,
    low_gate,
    high_gate,
    train_up,
    low_up,
    high_up,
    train_down,
    low_down,
    high_down,
    norm_train,
    norm_step,
):
    own_gate = (
        train_gate.astype(jnp.float32)
        + mix_rate * jnp.dot(low_gate, high_gate, preferred_element_type=jnp.float32)
    ).astype(jnp.bfloat16)
    own_up = (
        train_up.astype(jnp.float32)
        + mix_rate * jnp.dot(low_up, high_up, preferred_element_type=jnp.float32)
    ).astype(jnp.bfloat16)
    own_down = (
        train_down.astype(jnp.float32)
        + mix_rate * jnp.dot(low_down, high_down, preferred_element_type=jnp.float32)
    ).astype(jnp.bfloat16)
    owns = (own_gate, own_up, own_down.T)
    norm = (norm_train + norm_step).astype(jnp.bfloat16)[None]
    _, _, down, norms, gate, up = gather(owns, norm, rows, tp)
    return (gate, up, down, norms.reshape(-1))


def solution(mesh):
    in_specs = (
        P("rows", "tp"),
        P("rows", None),
        P(None, "tp"),
        P("rows", "tp"),
        P("rows", None),
        P(None, "tp"),
        P("tp", "rows"),
        P("tp", None),
        P(None, "rows"),
        P(("rows", "tp")),
        P(("rows", "tp")),
    )
    out_specs = (P("tp", None), P("tp", None), P(None, "tp"), P())
    return jax.shard_map(
        functools.partial(body, mesh.shape["rows"], mesh.shape["tp"]),
        mesh=mesh,
        in_specs=in_specs,
        out_specs=out_specs,
        check_vma=False,
    )
```
